128 devices in a mesh: ctx: 16 (over y, x), tp: 8 (over z, core).
Axes of the slice: x: 4, y: 4, z: 4, core: 2. Of those that a mesh axis runs over, the one named last changes fastest.
Arguments:
- queries: bfloat16 [8192, 64, 128], P('ctx', 'tp'), may hold values from -5 to 5
- own_keys: bfloat16 [8192, 8, 128], P('ctx', 'tp'), may hold values from -5 to 5
- own_values: bfloat16 [8192, 8, 128], P('ctx', 'tp'), may hold values from -5 to 5
- cache_keys: bfloat16 [8, 65536, 128], P('tp', 'ctx'), may hold values from -5 to 5
- cache_values: bfloat16 [8, 65536, 128], P('tp', 'ctx'), may hold values from -5 to 5
- selected: int32 [16, 8, 8], P('ctx', 'tp'), may hold values from 0 to 127, as said below
- out_weight: bfloat16 [8192, 8192], P('tp'), may hold values from -0.0625 to 0.0625
Outputs:
- mixed: bfloat16 [8192, 8192], P('ctx', 'tp')
The draws below stay inside these ranges and needn't reach their ends.
Inputs may be any that keep to these rules, and one draw needn't show every extreme that they name: `selected`: for each query block and key head, 8 different cache blocks, each lying in the cache of a different index of ctx (blocks k * 8 to (k + 1) * 8 - 1 for index k), so that at most 1 of them lie in one index.
All inputs are finite; a program needn't handle non-finite values.
Results may differ from the reference program's by a relative error of at most 0.017.
Values may be sent and summed in bfloat16 or wider, within the bound.
No kernel may reach another device: no remote copies, remote signals or barrier semaphores. Data moves between devices by JAX's collectives and lax.ppermute only.
A program may use at most 192 MiB of HBM per device.

```python
import jax
import jax.numpy as jnp
from jax import lax

D = 8192
HEADS = 64
KVH = 8
HD = 128
BLOCK = 512
TOPK = 8
CACHE_DEV = 4096
TOKENS = 8192
CACHE = 65536
N_TP = 8


def draw_queries(key, part):
    inner_key = jax.random.fold_in(key, 5)
    values_drawn = jnp.clip(jax.random.normal(inner_key, (TOKENS, HEADS, HD), jnp.float32), -5.0, 5.0)
    return values_drawn.astype(jnp.bfloat16)


def draw_own_keys(key, part):
    inner_key = jax.random.fold_in(key, 9)
    values_drawn = jnp.clip(jax.random.normal(inner_key, (TOKENS, KVH, HD), jnp.float32), -5.0, 5.0)
    return values_drawn.astype(jnp.bfloat16)


def draw_selected(key, part):
    row_count = TOKENS // BLOCK * KVH
    blocks_dev = CACHE_DEV // BLOCK
    owner_count = CACHE // CACHE_DEV
    row_keys = jax.random.split(jax.random.fold_in(key, 11), row_count)
    permuted = jax.vmap(lambda row_key: jax.random.permutation(row_key, owner_count))(row_keys)
    owner_of = permuted[:, :TOPK]
    inside = jax.random.randint(jax.random.fold_in(key, 13), (row_count, TOPK), 0, blocks_dev)
    chosen = owner_of * blocks_dev + inside
    return chosen.reshape(TOKENS // BLOCK, KVH, TOPK).astype(jnp.int32)


def level_of(key, dims, pieces, least, high):
    gain = 1.0
    for dim, parts in pieces:
        draws = jax.random.uniform(jax.random.fold_in(jax.random.fold_in(key, 6), dim), (parts,), jnp.float32, least / len(pieces), high / len(pieces))
        gain = gain * jnp.repeat(jnp.exp(draws), dims[dim] // parts).reshape((-1,) + (1,) * (len(dims) - 1 - dim))
    return gain


def noise(stream_key, dims, deviation, bound, cuts=(), held_as=jnp.bfloat16):
    factor_of = level_of(stream_key, dims, cuts, -0.22, 0.18) if cuts else 1.0
    entries = jax.random.normal(stream_key, dims, jnp.float32) * deviation * factor_of
    return jnp.minimum(jnp.maximum(entries, -bound), bound).astype(held_as)


def setup_inputs(seed: int = 0) -> dict:
    key_of = jax.random.split(jax.random.key(seed), 8)
    return {
        "queries": draw_queries(jax.random.fold_in(key_of[7], 71), 0),
        "own_keys": draw_own_keys(jax.random.fold_in(key_of[7], 71), 0),
        "own_values": noise(key_of[2], (TOKENS, KVH, HD), 1.0, 5.0, ((0, 16), (1, 8))),
        "cache_keys": noise(key_of[3], (KVH, CACHE, HD), 1.0, 5.0, ((0, 8), (1, 16))),
        "cache_values": noise(key_of[4], (KVH, CACHE, HD), 1.0, 5.0, ((0, 8), (1, 16))),
        "selected": draw_selected(jax.random.fold_in(key_of[7], 71), 0),
        "out_weight": noise(key_of[6], (D, D), D ** -0.5, 0.0625, ((0, 8),)),
    }


def attend(query_block, key_set, value_set):
    rows_count = query_block.shape[0]
    total_keys = key_set.shape[0]
    remote_count = total_keys - rows_count
    scores = jnp.einsum("tgd,kd->gtk", query_block.astype(jnp.float32), key_set.astype(jnp.float32))
    scores = scores * (query_block.shape[2] ** -0.5)
    column = lax.broadcasted_iota(jnp.int32, (rows_count, total_keys), 1)
    row_index = lax.broadcasted_iota(jnp.int32, (rows_count, total_keys), 0)
    allowed = (column < remote_count) | (column - remote_count <= row_index)
    scores = jnp.where(allowed[None], scores, -jnp.inf)
    largest = jnp.max(scores, axis=2, keepdims=True)
    powers = jnp.exp(scores - largest)
    weights = (powers / jnp.sum(powers, axis=2, keepdims=True)).astype(jnp.bfloat16)
    mixed_heads = jnp.einsum("gtk,kd->tgd", weights.astype(jnp.float32), value_set.astype(jnp.float32))
    return mixed_heads.astype(jnp.bfloat16)


def reference(queries, own_keys, own_values, cache_keys, cache_values, selected, out_weight):
    group_size = HEADS // KVH
    block_count = CACHE // BLOCK
    key_table = cache_keys.reshape(KVH, block_count, BLOCK, HD)
    value_table = cache_values.reshape(KVH, block_count, BLOCK, HD)

    def one_block(block_index):
        start = block_index * BLOCK
        query_block = lax.dynamic_slice_in_dim(queries, start, BLOCK, 0)
        block_keys = lax.dynamic_slice_in_dim(own_keys, start, BLOCK, 0)
        block_values = lax.dynamic_slice_in_dim(own_values, start, BLOCK, 0)
        chosen_all = selected[block_index]
        outputs = []
        for kv_head in range(KVH):
            chosen_ids = chosen_all[kv_head]
            key_set = jnp.concatenate([key_table[kv_head][chosen_ids].reshape(TOPK * BLOCK, HD), block_keys[:, kv_head]], axis=0)
            value_set = jnp.concatenate([value_table[kv_head][chosen_ids].reshape(TOPK * BLOCK, HD), block_values[:, kv_head]], axis=0)
            outputs.append(attend(query_block[:, kv_head * group_size:(kv_head + 1) * group_size], key_set, value_set))
        return jnp.concatenate(outputs, axis=1)

    attended = lax.map(one_block, jnp.arange(TOKENS // BLOCK, dtype=jnp.int32))
    attended = attended.reshape(TOKENS, D)
    share_rows = D // N_TP
    total_sum = jnp.zeros((TOKENS, D), jnp.float32)
    for group_index in range(N_TP):
        partial_value = jnp.dot(attended[:, group_index * share_rows:(group_index + 1) * share_rows], out_weight[group_index * share_rows:(group_index + 1) * share_rows], preferred_element_type=jnp.float32).astype(jnp.bfloat16)
        partial_value = lax.optimization_barrier(partial_value)
        total_sum = total_sum + partial_value.astype(jnp.float32)
    return total_sum.astype(jnp.bfloat16)
```

```python
import functools, math
import jax, jax.numpy as jnp
from jax import lax
from jax.experimental import pallas as pl
from jax.experimental.pallas import tpu as pltpu
from jax.sharding import PartitionSpec as P

C = 128 ** -0.5 * math.log2(math.e)
R = 512
H = 8


def attn_body(pos_ref, q_ref, k_ref, v_ref, *rest, sub, per, items, unroll, first, last, causal):
    rest = list(rest)
    if not first:
        acc_in, m_in = rest.pop(0), rest.pop(0)
    if last:
        o_ref = rest.pop(0)
        acc_ref, m_ref, s_ref = rest
    else:
        acc_ref, m_ref, s_ref = rest
    total = H * items
    ones = jnp.ones((sub, 128), jnp.bfloat16)

    def slot(j, i):
        return pos_ref[j * per + i]

    def scores(t, buf):
        h, j = t // items, t % items
        q = q_ref[h]
        for i in range(per):
            s_ref[buf, :, i * sub:(i + 1) * sub] = lax.dot_general(
                q, k_ref[slot(j, i)], (((1,), (1,)), ((), ())), preferred_element_type=jnp.float32)

    def step(t, buf, j_static):
        h, j = t // items, t % items
        s = s_ref[buf]
        if causal:
            row = lax.broadcasted_iota(jnp.int32, s.shape, 0)
            col = lax.broadcasted_iota(jnp.int32, s.shape, 1)
            s = jnp.where(col <= row, s, -1e30)
        m_blk = jnp.max(s, axis=1, keepdims=True)
        fresh = first and j_static == 0
        if fresh:
            m_new = jnp.broadcast_to(m_blk, (R, 128))
        else:
            m_old = m_in[h] if j_static == 0 else m_ref[h]
            m_new = jnp.maximum(m_old, m_blk)
        mc = m_new[:, :1] * C
        p = jnp.exp2(s * C - mc).astype(jnp.bfloat16)
        pv = None
        for i in range(per):
            ve = jnp.concatenate([v_ref[slot(j, i)], ones], axis=1)
            d = jnp.dot(p[:, i * sub:(i + 1) * sub], ve, preferred_element_type=jnp.float32)
            pv = d if pv is None else pv + d
        if not fresh:
            alpha = jnp.exp2((m_old - m_new) * C)
            a_old = acc_in[h] if j_static == 0 else acc_ref[h]
            pv = jnp.concatenate([a_old[:, :128] * alpha, a_old[:, 128:] * alpha], axis=1) + pv
        if last and j_static == items - 1:
            o_ref[:, pl.ds(pl.multiple_of(h * 128, 128), 128)] = (pv[:, :128] / pv[:, 128:]).astype(jnp.bfloat16)
        else:
            acc_ref[h] = pv
            m_ref[h] = m_new

    scores(0, 0)

    def body(g, _):
        for u in range(unroll):
            t = g * unroll + u
            scores(jnp.minimum(t + 1, total - 1), (u + 1) % 2)
            step(t, u % 2, u % items)
        return 0

    lax.fori_loop(0, total // unroll, body, 0)


def attn_call(pos, q, k, v, state=None, *, sub, per, items, unroll, last, causal=False):
    first = state is None
    kern = functools.partial(attn_body, sub=sub, per=per, items=items, unroll=unroll, first=first, last=last, causal=causal)
    vm = pl.BlockSpec(memory_space=pltpu.VMEM)
    keys = sub * per * items
    acc_s = jax.ShapeDtypeStruct((H, R, 256), jnp.float32)
    m_s = jax.ShapeDtypeStruct((H, R, 128), jnp.float32)
    args = [q, k, v]
    if not first:
        args += list(state)
    scr = [pltpu.VMEM((2, R, sub * per), jnp.float32)]
    if last:
        out_shape = jax.ShapeDtypeStruct((R, H * 128), jnp.bfloat16)
        out_specs = vm
        scr = [pltpu.VMEM((H, R, 256), jnp.float32), pltpu.VMEM((H, R, 128), jnp.float32)] + scr
    else:
        out_shape = (acc_s, m_s)
        out_specs = (vm, vm)
    return pl.pallas_call(
        kern, out_shape=out_shape,
        in_specs=[pl.BlockSpec(memory_space=pltpu.SMEM)] + [vm] * len(args), out_specs=out_specs,
        scratch_shapes=scr,
        compiler_params=pltpu.CompilerParams(vmem_limit_bytes=56 * 2**20),
        cost_estimate=pl.CostEstimate(flops=4 * H * R * keys * 128 , bytes_accessed=2 * keys * 256, transcendentals=H * R * keys),
    )(pos, *args)


def shards(queries, own_keys, own_values, cache_keys, cache_values, selected, out_weight):
    blocks_dev = cache_keys.shape[1] // R
    picked = selected[0, 0]
    owners = lax.axis_size("ctx")
    owner_of = picked // blocks_dev
    inside = picked % blocks_dev
    match = owner_of[:, None] == jnp.arange(owners, dtype=jnp.int32)[None, :]
    request = jnp.sum(jnp.where(match, inside[:, None], 0), axis=0)
    wanted = lax.all_to_all(request, "ctx", split_axis=0, concat_axis=0, tiled=True)
    flat_keys = cache_keys.reshape(blocks_dev, R, 128)
    flat_values = cache_values.reshape(blocks_dev, R, 128)
    got_keys = lax.all_to_all(flat_keys[wanted], "ctx", split_axis=0, concat_axis=0, tiled=True)
    got_values = lax.all_to_all(flat_values[wanted], "ctx", split_axis=0, concat_axis=0, tiled=True)
    q = jnp.transpose(queries, (1, 0, 2))
    zero = jnp.zeros((1,), jnp.int32)
    state = attn_call(zero, q, own_keys.reshape(1, R, 128), own_values.reshape(1, R, 128),
                      sub=512, per=1, items=1, unroll=2, last=False, causal=True)
    attended = attn_call(owner_of, q, got_keys, got_values, state,
                         sub=512, per=2, items=4, unroll=4, last=True)
    partial_term = jnp.dot(attended, out_weight, preferred_element_type=jnp.float32).astype(jnp.bfloat16)
    return lax.psum_scatter(partial_term, "tp", scatter_dimension=1, tiled=True)


def solution(mesh):
    in_specs = (
        P("ctx", "tp", None),
        P("ctx", "tp", None),
        P("ctx", "tp", None),
        P("tp", "ctx", None),
        P("tp", "ctx", None),
        P("ctx", "tp", None),
        P("tp", None),
    )
    return jax.shard_map(shards, mesh=mesh, in_specs=in_specs, out_specs=P("ctx", "tp"), check_vma=False)
```

```python
import functools
import math

import jax
import jax.numpy as jnp
from jax import lax
from jax.experimental import pallas as pl
from jax.experimental.pallas import tpu as pltpu
from jax.sharding import PartitionSpec as P


C = 128 ** -0.5 * math.log2(math.e)
R = 512
H = 8
W = 128
CUT = 320
ATT = 58
MIB = 2**20
VM = pl.BlockSpec(memory_space=pltpu.VMEM)
SM = pl.BlockSpec(memory_space=pltpu.SMEM)


def cat(parts, axis):
    return parts[0] if len(parts) == 1 else jnp.concatenate(parts, axis=axis)


def attend_body(pos_ref, q_ref, *rest, per, items, group, own, last):
    rest = list(rest)
    if own:
        k_ref, v_ref = rest.pop(0), rest.pop(0)
    else:
        kv_ref, acc_in, m_in = rest.pop(0), rest.pop(0), rest.pop(0)
    if last:
        o_ref = rest.pop(0)
    acc_ref, m_ref, s_ref = rest
    g = pl.program_id(0)
    keys = s_ref.shape[2]
    steps = group * items

    def chunk(j, which):
        if own:
            return (v_ref if which else k_ref)[...]
        return cat([kv_ref[pos_ref[j * per + i], which] for i in range(per)], 0)

    def scores(head, j, buf):
        s_ref[buf] = lax.dot_general(
            q_ref[head], chunk(j, 0), (((1,), (1,)), ((), ())), preferred_element_type=jnp.float32
        )

    def step(r, j, buf):
        s = s_ref[buf]
        if own:
            row = lax.broadcasted_iota(jnp.int32, s.shape, 0)
            col = lax.broadcasted_iota(jnp.int32, s.shape, 1)
            s = jnp.where(col <= row, s, -1e30)
        m_blk = jnp.max(s, axis=1, keepdims=True)
        if own:
            m_new = jnp.broadcast_to(m_blk, (R, W))
        else:
            m_old = m_in[r] if j == 0 else m_ref[r]
            m_new = jnp.maximum(m_old, m_blk)
        p = jnp.exp2(s * C - m_new[:, :1] * C).astype(jnp.bfloat16)
        ve = jnp.concatenate([chunk(j, 1), jnp.ones((keys, W), jnp.bfloat16)], axis=1)
        pv = jnp.dot(p, ve, preferred_element_type=jnp.float32)
        if not own:
            alpha = jnp.exp2((m_old - m_new) * C)
            a_old = acc_in[r] if j == 0 else acc_ref[r]
            pv = jnp.concatenate([a_old[:, :W] * alpha, a_old[:, W:] * alpha], axis=1) + pv
        if last and j == items - 1:
            o_ref[:, r * W : (r + 1) * W] = (pv[:, :W] / pv[:, W:]).astype(jnp.bfloat16)
        else:
            acc_ref[r] = pv
            m_ref[r] = m_new

    @pl.when(g == 0)
    def _():
        scores(0, 0, 0)

    for u in range(steps):
        if u + 1 < steps:
            scores(g * group + (u + 1) // items, (u + 1) % items, (u + 1) % 2)
        else:
            scores(jnp.minimum((g + 1) * group, H - 1), 0, (u + 1) % 2)
        step(u // items, u % items, u % 2)


def attend(pos, q, arrays, *, per, items, width, group=2, own=False, last=False):
    keys = per * width
    acc = pl.BlockSpec((group, R, 2 * W), lambda g: (g, 0, 0))
    top = pl.BlockSpec((group, R, W), lambda g: (g, 0, 0))
    scratch = [pltpu.VMEM((2, R, keys), jnp.float32)]
    if last:
        out_shape = jax.ShapeDtypeStruct((R, H * W), jnp.bfloat16)
        out_specs = pl.BlockSpec((R, group * W), lambda g: (0, g))
        scratch = [pltpu.VMEM((group, R, 2 * W), jnp.float32), pltpu.VMEM((group, R, W), jnp.float32)] + scratch
    else:
        out_shape = (jax.ShapeDtypeStruct((H, R, 2 * W), jnp.float32), jax.ShapeDtypeStruct((H, R, W), jnp.float32))
        out_specs = (acc, top)
    return pl.pallas_call(
        functools.partial(attend_body, per=per, items=items, group=group, own=own, last=last),
        grid=(H // group,),
        out_shape=out_shape,
        in_specs=[SM, VM] + ([VM, VM] if own else [VM, acc, top]),
        out_specs=out_specs,
        scratch_shapes=scratch,
        compiler_params=pltpu.CompilerParams(vmem_limit_bytes=ATT * MIB),
        cost_estimate=pl.CostEstimate(
            flops=16 * H * R * keys * items * W, bytes_accessed=16 * MIB, transcendentals=H * R * keys * items
        ),
    )(pos, q, *arrays)


def gather_body(want_ref, k_ref, v_ref, a_ref, b_ref, sems):
    copies = []
    for i in range(a_ref.shape[0]):
        for which, ref in enumerate((k_ref, v_ref)):
            block = ref.at[want_ref[i]]
            copies.append(pltpu.make_async_copy(block.at[pl.ds(0, CUT)], a_ref.at[i, which], sems.at[i, which, 0]))
            copies.append(pltpu.make_async_copy(block.at[pl.ds(CUT, R - CUT)], b_ref.at[i, which], sems.at[i, which, 1]))
    for copy in copies:
        copy.start()
    for copy in copies:
        copy.wait()


def gather(want, keys, values):
    n = want.shape[0]
    hbm = pl.BlockSpec(memory_space=pltpu.HBM)
    return pl.pallas_call(
        gather_body,
        out_shape=(
            jax.ShapeDtypeStruct((n, 2, CUT, W), jnp.bfloat16),
            jax.ShapeDtypeStruct((n, 2, R - CUT, W), jnp.bfloat16),
        ),
        in_specs=[SM, VM, VM],
        out_specs=(hbm, hbm),
        scratch_shapes=[pltpu.SemaphoreType.DMA((n, 2, 2))],
        compiler_params=pltpu.CompilerParams(vmem_limit_bytes=16 * MIB),
        cost_estimate=pl.CostEstimate(flops=0, bytes_accessed=8 * MIB, transcendentals=0),
    )(want, keys, values)


def copy_body(ix_ref, i_ref, o_ref):
    o_ref[...] = i_ref[...]


def sibling_columns(weight, side):
    rows = weight.shape[0]
    return pl.pallas_call(
        copy_body,
        grid_spec=pltpu.PrefetchScalarGridSpec(
            num_scalar_prefetch=1,
            grid=(4,),
            in_specs=[pl.BlockSpec((rows, 1024), lambda n, ix: (0, 2 * n + ix[0]))],
            out_specs=pl.BlockSpec((rows, 1024), lambda n, ix: (0, n)),
        ),
        out_shape=jax.ShapeDtypeStruct((rows, 4096), jnp.bfloat16),
        compiler_params=pltpu.CompilerParams(vmem_limit_bytes=60 * MIB),
        cost_estimate=pl.CostEstimate(flops=0, bytes_accessed=16 * MIB, transcendentals=0),
    )(side, weight)


def project_body(j_ref, a_ref, b_ref, w_ref, ws_ref, *rest, pieces, received):
    outs = rest[received : received + 2]
    buf, sems = rest[received + 2 :]
    z, c = j_ref[0] // 2, j_ref[0] % 2

    def fetch(n, part):
        d, half = pieces[n // 2]
        zz = (z + d) % 4
        ref = ws_ref if part else w_ref
        first = zz * 4 + 2 * half if part else (2 * zz + c) * 4 + 2 * half
        start = pl.multiple_of((first + n % 2) * 256, 256)
        return pltpu.make_async_copy(ref.at[:, pl.ds(start, 256)], buf.at[n, part], sems.at[n, part])

    for n in range(4):
        for part in range(2):
            fetch(n, part).start()
    for half in range(2):

        def one(m, carry):
            n = half * 2 + m
            for part in range(2):
                pltpu.make_async_copy(w_ref.at[:, pl.ds(0, 256)], buf.at[n, part], sems.at[n, part]).wait()
            cols = pl.ds(pl.multiple_of(m * 256, 256), 256)
            r = jnp.dot(a_ref[...], buf[n, 0], preferred_element_type=jnp.float32)
            r = r + jnp.dot(b_ref[...], buf[n, 1], preferred_element_type=jnp.float32)
            if received:
                r = r + rest[half][:, cols].astype(jnp.float32)
            outs[half][:, cols] = r.astype(outs[half].dtype)
            return carry

        lax.fori_loop(0, 2, one, 0)


def project(pieces, j, a, b, w, ws, recv=(), dtype=jnp.bfloat16):
    rows, depth = a.shape
    hbm = pl.BlockSpec(memory_space=pltpu.HBM)
    return pl.pallas_call(
        functools.partial(project_body, pieces=pieces, received=len(recv)),
        out_shape=[jax.ShapeDtypeStruct((rows, 512), dtype)] * 2,
        in_specs=[SM, VM, VM, hbm, hbm] + [VM] * len(recv),
        out_specs=[VM, VM],
        scratch_shapes=[pltpu.VMEM((4, 2, depth, 256), jnp.bfloat16), pltpu.SemaphoreType.DMA((4, 2))],
        compiler_params=pltpu.CompilerParams(vmem_limit_bytes=60 * MIB),
        cost_estimate=pl.CostEstimate(flops=4 * rows * depth * 1024, bytes_accessed=7 * MIB, transcendentals=0),
    )(j, a, b, w, ws, *recv)


def move(a, f):
    return lax.ppermute(a, "tp", [(j, f(j)) for j in range(8)])


def up(a):
    return move(a, lambda j: (j + 2) % 8)


def down(a):
    return move(a, lambda j: (j - 2) % 8)


def swap(a):
    return move(a, lambda j: j ^ 1)


def tail(att, weight, theirs):
    j = lax.axis_index("tp").reshape(1)
    other = swap(att)
    args = (j, att, other, weight, theirs)
    c2a, c2b = project(((2, 0), (2, 1)), *args)
    a2, b2 = up(c2a), down(c2b)
    c1b, c3a = project(((1, 1), (3, 0)), *args)
    u2, d2 = up(c1b), down(c3a)
    c1a, c3b = project(((1, 0), (3, 1)), *args, recv=(a2, b2))
    u1, d1 = up(c1a), down(c3b)
    left, right = project(((0, 0), (0, 1)), *args, recv=(d2, u2), dtype=jnp.float32)
    left = left + u1.astype(jnp.float32)
    right = right + d1.astype(jnp.float32)
    return jnp.concatenate([left, right], axis=1).astype(jnp.bfloat16)


def shards(queries, own_keys, own_values, cache_keys, cache_values, selected, out_weight):
    blocks_dev = cache_keys.shape[1] // R
    picked = selected[0, 0]
    owners = lax.axis_size("ctx")
    owner_of = picked // blocks_dev
    inside = picked % blocks_dev
    match = owner_of[:, None] == jnp.arange(owners, dtype=jnp.int32)[None, :]
    request = jnp.sum(jnp.where(match, inside[:, None], 0), axis=0)
    wanted = lax.all_to_all(request, "ctx", split_axis=0, concat_axis=0, tiled=True)
    send_a, send_b = gather(wanted, cache_keys.reshape(blocks_dev, R, W), cache_values.reshape(blocks_dev, R, W))
    got_a = lax.all_to_all(send_a, "ctx", split_axis=0, concat_axis=0, tiled=True)
    got_a, send_b = lax.optimization_barrier((got_a, send_b))
    got_b = lax.all_to_all(send_b, "ctx", split_axis=0, concat_axis=0, tiled=True)
    side = (1 - lax.axis_index("tp") % 2).reshape(1)
    theirs = sibling_columns(out_weight, side)
    theirs = swap(theirs)
    q = jnp.transpose(queries, (1, 0, 2))
    zero = jnp.zeros((1,), jnp.int32)
    state = attend(zero, q, (own_keys.reshape(R, W), own_values.reshape(R, W)), per=1, items=1, width=R, own=True)
    state = attend(owner_of, q, (got_a, *state), per=4, items=2, width=CUT)
    att = attend(owner_of, q, (got_b, *state), per=4, items=2, width=R - CUT, last=True)
    return tail(att, out_weight, theirs)


def solution(mesh):
    in_specs = (
        P("ctx", "tp", None),
        P("ctx", "tp", None),
        P("ctx", "tp", None),
        P("tp", "ctx", None),
        P("tp", "ctx", None),
        P("ctx", "tp", None),
        P("tp", None),
    )
    return jax.shard_map(shards, mesh=mesh, in_specs=in_specs, out_specs=P("ctx", "tp"), check_vma=False)
```

```python
import functools
import math

import jax
import jax.numpy as jnp
from jax import lax
from jax.experimental import pallas as pl
from jax.experimental.pallas import tpu as pltpu
from jax.sharding import PartitionSpec as P


C = 128 ** -0.5 * math.log2(math.e)
R = 512
H = 8
W = 128
CUT = 320
BLOCKS = 8
ATT = 58
LAST = 58
PROJ = 50
MIB = 2**20
VM = pl.BlockSpec(memory_space=pltpu.VMEM)
SM = pl.BlockSpec(memory_space=pltpu.SMEM)
HBM = pl.BlockSpec(memory_space=pltpu.HBM)


def cat(parts, axis):
    return parts[0] if len(parts) == 1 else jnp.concatenate(parts, axis=axis)


def attend_body(pos_ref, q_ref, *rest, per, items, group, own, last):
    rest = list(rest)
    if own:
        k_ref, v_ref = rest.pop(0), rest.pop(0)
    else:
        kv_ref, acc_in, m_in = rest.pop(0), rest.pop(0), rest.pop(0)
    if last:
        o_ref = rest.pop(0)
    acc_ref, m_ref, s_ref = rest
    g = pl.program_id(0)
    keys = s_ref.shape[2]
    steps = group * items

    def chunk(j, which):
        if own:
            return (v_ref if which else k_ref)[...]
        return cat([kv_ref[pos_ref[j * per + i] // BLOCKS, which] for i in range(per)], 0)

    def scores(head, j, buf):
        s_ref[buf] = lax.dot_general(
            q_ref[head], chunk(j, 0), (((1,), (1,)), ((), ())), preferred_element_type=jnp.float32
        )

    def step(r, j, buf):
        s = s_ref[buf]
        if own:
            row = lax.broadcasted_iota(jnp.int32, s.shape, 0)
            col = lax.broadcasted_iota(jnp.int32, s.shape, 1)
            s = jnp.where(col <= row, s, -1e30)
        m_blk = jnp.max(s, axis=1, keepdims=True)
        if own:
            m_new = jnp.broadcast_to(m_blk, (R, W))
        else:
            m_old = m_in[r] if j == 0 else m_ref[r]
            m_new = jnp.maximum(m_old, m_blk)
        p = jnp.exp2(s * C - m_new[:, :1] * C).astype(jnp.bfloat16)
        ve = jnp.concatenate([chunk(j, 1), jnp.ones((keys, W), jnp.bfloat16)], axis=1)
        pv = jnp.dot(p, ve, preferred_element_type=jnp.float32)
        if not own:
            alpha = jnp.exp2((m_old - m_new) * C)
            a_old = acc_in[r] if j == 0 else acc_ref[r]
            pv = jnp.concatenate([a_old[:, :W] * alpha, a_old[:, W:] * alpha], axis=1) + pv
        if last and j == items - 1:
            o_ref[:, r * W : (r + 1) * W] = (pv[:, :W] / pv[:, W:]).astype(jnp.bfloat16)
        else:
            acc_ref[r] = pv
            m_ref[r] = m_new

    @pl.when(g == 0)
    def _():
        scores(0, 0, 0)

    for u in range(steps):
        if u + 1 < steps:
            scores(g * group + (u + 1) // items, (u + 1) % items, (u + 1) % 2)
        else:
            scores(jnp.minimum((g + 1) * group, H - 1), 0, (u + 1) % 2)
        step(u // items, u % items, u % 2)


def attend(pos, q, arrays, *, per, items, width, group=2, own=False, last=False):
    keys = per * width
    acc = pl.BlockSpec((group, R, 2 * W), lambda g: (g, 0, 0))
    top = pl.BlockSpec((group, R, W), lambda g: (g, 0, 0))
    scratch = [pltpu.VMEM((2, R, keys), jnp.float32)]
    if last:
        out_shape = jax.ShapeDtypeStruct((R, H * W), jnp.bfloat16)
        out_specs = pl.BlockSpec((R, group * W), lambda g: (0, g))
        scratch = [pltpu.VMEM((group, R, 2 * W), jnp.float32), pltpu.VMEM((group, R, W), jnp.float32)] + scratch
    else:
        out_shape = (jax.ShapeDtypeStruct((H, R, 2 * W), jnp.float32), jax.ShapeDtypeStruct((H, R, W), jnp.float32))
        out_specs = (acc, top)
    return pl.pallas_call(
        functools.partial(attend_body, per=per, items=items, group=group, own=own, last=last),
        grid=(H // group,),
        out_shape=out_shape,
        in_specs=[SM, VM] + ([VM, VM] if own else [VM, acc, top]),
        out_specs=out_specs,
        scratch_shapes=scratch,
        compiler_params=pltpu.CompilerParams(vmem_limit_bytes=(LAST if last else ATT) * MIB),
        cost_estimate=pl.CostEstimate(
            flops=16 * H * R * keys * items * W, bytes_accessed=16 * MIB, transcendentals=H * R * keys * items
        ),
    )(pos, q, *arrays)


def request_body(pick_ref, o_ref):
    o_ref[...] = jnp.zeros_like(o_ref)
    for k in range(pick_ref.shape[0]):
        o_ref[pick_ref[k] // BLOCKS] = jnp.full((1, W), pick_ref[k] % BLOCKS, jnp.int32)


def request(picked, owners):
    return pl.pallas_call(
        request_body,
        out_shape=jax.ShapeDtypeStruct((owners, 1, W), jnp.int32),
        in_specs=[SM],
        out_specs=VM,
    )(picked)


def gather_body(want_ref, k_ref, v_ref, o_ref, buf, in_sems, out_sems, *, first, rows):
    loads, stores = [], []
    for which, ref in enumerate((k_ref, v_ref)):
        loads.append(pltpu.make_async_copy(ref.at[:, pl.ds(first, rows)], buf.at[which], in_sems.at[which]))
        for i in range(o_ref.shape[0]):
            stores.append(pltpu.make_async_copy(buf.at[which, want_ref[i, 0, 0]], o_ref.at[i, which], out_sems.at[which, i]))
    n = o_ref.shape[0]
    for load in loads:
        load.start()
    for which in range(2):
        loads[which].wait()
        for store in stores[which * n : which * n + n]:
            store.start()
    for store in stores:
        store.wait()


def gather(want, keys, values, first, rows):
    n = want.shape[0]
    return pl.pallas_call(
        functools.partial(gather_body, first=first, rows=rows),
        out_shape=jax.ShapeDtypeStruct((n, 2, rows, W), jnp.bfloat16),
        in_specs=[SM, HBM, HBM],
        out_specs=HBM,
        scratch_shapes=[
            pltpu.VMEM((2, keys.shape[0], rows, W), jnp.bfloat16),
            pltpu.SemaphoreType.DMA((2,)),
            pltpu.SemaphoreType.DMA((2, n)),
        ],
        compiler_params=pltpu.CompilerParams(vmem_limit_bytes=60 * MIB),
        cost_estimate=pl.CostEstimate(flops=0, bytes_accessed=5 * MIB, transcendentals=0),
    )(want, keys, values)


def copy_body(ix_ref, i_ref, o_ref):
    o_ref[...] = i_ref[...]


def sibling_columns(weight, side):
    rows = weight.shape[0]
    return pl.pallas_call(
        copy_body,
        grid_spec=pltpu.PrefetchScalarGridSpec(
            num_scalar_prefetch=1,
            grid=(4,),
            in_specs=[pl.BlockSpec((rows, 1024), lambda n, ix: (0, 2 * n + ix[0]))],
            out_specs=pl.BlockSpec((rows, 1024), lambda n, ix: (0, n)),
        ),
        out_shape=jax.ShapeDtypeStruct((rows, 4096), jnp.bfloat16),
        compiler_params=pltpu.CompilerParams(vmem_limit_bytes=60 * MIB),
        cost_estimate=pl.CostEstimate(flops=0, bytes_accessed=16 * MIB, transcendentals=0),
    )(side, weight)


def project_body(j_ref, a_ref, b_ref, w_ref, ws_ref, *rest, pieces, received):
    outs = rest[received : received + 2]
    buf, sems = rest[received + 2 :]
    z, c = j_ref[0] // 2, j_ref[0] % 2

    def fetch(n, part):
        d, side = pieces[n // 2]
        zz = (z + d) % 4
        first = zz if part else 2 * zz + c
        start = pl.multiple_of((first * 4 + 2 * side + n % 2) * 256, 256)
        ref = ws_ref if part else w_ref
        return pltpu.make_async_copy(ref.at[:, pl.ds(start, 256)], buf.at[n, part], sems.at[n, part])

    for n in range(4):
        for part in range(2):
            fetch(n, part).start()
    for half in range(2):

        def one(m, carry):
            n = half * 2 + m
            for part in range(2):
                pltpu.make_async_copy(w_ref.at[:, pl.ds(0, 256)], buf.at[n, part], sems.at[n, part]).wait()
            cols = pl.ds(pl.multiple_of(m * 256, 256), 256)
            r = jnp.dot(a_ref[...], buf[n, 0], preferred_element_type=jnp.float32)
            r = r + jnp.dot(b_ref[...], buf[n, 1], preferred_element_type=jnp.float32)
            if received:
                r = r + rest[half][:, cols].astype(jnp.float32)
            outs[half][:, cols] = r.astype(outs[half].dtype)
            return carry

        lax.fori_loop(0, 2, one, 0)


def project(pieces, j, a, b, w, ws, recv=(), dtype=jnp.bfloat16):
    rows, depth = a.shape
    return pl.pallas_call(
        functools.partial(project_body, pieces=pieces, received=len(recv)),
        out_shape=[jax.ShapeDtypeStruct((rows, 512), dtype)] * 2,
        in_specs=[SM, VM, VM, HBM, HBM] + [VM] * len(recv),
        out_specs=[VM, VM],
        scratch_shapes=[pltpu.VMEM((4, 2, depth, 256), jnp.bfloat16), pltpu.SemaphoreType.DMA((4, 2))],
        compiler_params=pltpu.CompilerParams(vmem_limit_bytes=PROJ * MIB),
        cost_estimate=pl.CostEstimate(flops=4 * rows * depth * 1024, bytes_accessed=7 * MIB, transcendentals=0),
    )(j, a, b, w, ws, *recv)


def close_body(l_ref, u_ref, r_ref, d_ref, o_ref):
    o_ref[:, :512] = (l_ref[...] + u_ref[...].astype(jnp.float32)).astype(jnp.bfloat16)
    o_ref[:, 512:] = (r_ref[...] + d_ref[...].astype(jnp.float32)).astype(jnp.bfloat16)


def close(left, u1, right, d1):
    return pl.pallas_call(
        close_body,
        out_shape=jax.ShapeDtypeStruct((R, 1024), jnp.bfloat16),
        in_specs=[VM] * 4,
        out_specs=VM,
        compiler_params=pltpu.CompilerParams(vmem_limit_bytes=16 * MIB),
        cost_estimate=pl.CostEstimate(flops=R * 1024, bytes_accessed=4 * MIB, transcendentals=0),
    )(left, u1, right, d1)


def move(a, f):
    return lax.ppermute(a, "tp", [(j, f(j)) for j in range(8)])


def up(a):
    return move(a, lambda j: (j + 2) % 8)


def down(a):
    return move(a, lambda j: (j - 2) % 8)


def swap(a):
    return move(a, lambda j: j ^ 1)


def tail(j, att, weight, theirs):
    other = swap(att)
    args = (j, att, other, weight, theirs)
    c2a, c2b = project(((2, 0), (2, 1)), *args)
    a2, b2 = up(c2a), down(c2b)
    c1b, c3a = project(((1, 1), (3, 0)), *args)
    u2, d2 = up(c1b), down(c3a)
    c1a, c3b = project(((1, 0), (3, 1)), *args, recv=(a2, b2))
    u1, d1 = up(c1a), down(c3b)
    left, right = project(((0, 0), (0, 1)), *args, recv=(d2, u2), dtype=jnp.float32)
    return close(left, u1, right, d1)


def shards(queries, own_keys, own_values, cache_keys, cache_values, selected, out_weight):
    picked = selected[0, 0]
    asked = request(picked, lax.axis_size("ctx"))
    wanted = lax.all_to_all(asked, "ctx", split_axis=0, concat_axis=0, tiled=True)
    caches = cache_keys.reshape(BLOCKS, R, W), cache_values.reshape(BLOCKS, R, W)
    send_a = gather(wanted, *caches, 0, CUT)
    send_b = gather(wanted, *caches, CUT, R - CUT)
    got_a = lax.all_to_all(send_a, "ctx", split_axis=0, concat_axis=0, tiled=True)
    got_a, send_b = lax.optimization_barrier((got_a, send_b))
    got_b = lax.all_to_all(send_b, "ctx", split_axis=0, concat_axis=0, tiled=True)
    j = lax.axis_index("tp").reshape(1)
    theirs = sibling_columns(out_weight, 1 - j % 2)
    theirs = swap(theirs)
    q = jnp.transpose(queries, (1, 0, 2))
    zero = jnp.zeros((1,), jnp.int32)
    state = attend(zero, q, (own_keys.reshape(R, W), own_values.reshape(R, W)), per=1, items=1, width=R, own=True)
    state = attend(picked, q, (got_a, *state), per=4, items=2, width=CUT)
    att = attend(picked, q, (got_b, *state), per=4, items=2, width=R - CUT, group=4, last=True)
    return tail(j, att, out_weight, theirs)


def solution(mesh):
    in_specs = (
        P("ctx", "tp", None),
        P("ctx", "tp", None),
        P("ctx", "tp", None),
        P("tp", "ctx", None),
        P("tp", "ctx", None),
        P("ctx", "tp", None),
        P("tp", None),
    )
    return jax.shard_map(shards, mesh=mesh, in_specs=in_specs, out_specs=P("ctx", "tp"), check_vma=False)
```
